32 devices in a mesh: replica: 4 (over x, core), fsdp: 8 (over z, y).
Axes of the slice: x: 2, y: 2, z: 4, core: 2. Of those that a mesh axis runs over, the one named last changes fastest.
Arguments:
- anchor: float32 [1536, 1536], P('fsdp', 'replica'), may hold values from -0.15625 to 0.15625
- momentum: float32 [1536, 1536], P('fsdp', 'replica'), may hold values from -0.75 to 0.75
- change: float32 [4, 1536, 1536], P('replica', 'fsdp'), may hold values from -0.75 to 0.75
- adam_first: float32 [4, 1536, 1536], P('replica', 'fsdp'), may hold values from -4 to 4
- adam_second: float32 [4, 1536, 1536], P('replica', 'fsdp'), may hold values from 0.1 to 2
- attn_out: bfloat16 [4, 8192, 1536], P('replica', 'fsdp'), may hold values from -6 to 6
- grad_out: bfloat16 [4, 8192, 1536], P('replica', 'fsdp'), may hold values from -6 to 6
Outputs:
- new_anchor: float32 [1536, 1536], P('fsdp', 'replica')
- new_momentum: float32 [1536, 1536], P('fsdp', 'replica')
- new_local: float32 [4, 1536, 1536], P('replica', 'fsdp')
- new_first: float32 [4, 1536, 1536], P('replica', 'fsdp')
- new_second: float32 [4, 1536, 1536], P('replica', 'fsdp')
- input_grad: bfloat16 [4, 8192, 1536], P('replica', 'fsdp')
The draws below stay inside these ranges and needn't reach their ends.
All inputs are finite; a program needn't handle non-finite values.
Results may differ from the reference program's by a relative error of at most 0.0049.
Values may be sent and summed in bfloat16 or wider, within the bound.
A program may use at most 128 MiB of HBM per device.

```python
import math
import jax
import jax.numpy as jnp
from jax import lax

D = 1536
REPLICAS = 4
TOKENS = 8192


def spiked(values, key, source, target, shards_of, factor):
    owner, partner = [(jnp.arange(values.shape[dim]) // (values.shape[dim] // shards_of)).reshape([-1 if axis == dim else 1 for axis in range(values.ndim)]) for dim in (source, target)]
    chosen = jax.random.permutation(key, shards_of)[partner]
    strong = (owner == chosen) | (owner == (partner + shards_of // 2) % shards_of)
    return jnp.where(strong, factor * values, values)


def shard_levels(own_key, dims, split, smallest, top_value):
    gain, own = 1.0, jax.random.fold_in(own_key, 6)
    for position, shards_of in split:
        steps = jnp.exp(jax.random.uniform(jax.random.fold_in(own, position), (shards_of,), jnp.float32, smallest / len(split), top_value / len(split)))
        gain = gain * jnp.repeat(steps, dims[position] // shards_of).reshape([-1 if axis == position else 1 for axis in range(len(dims))])
    return gain


def gaussian(own_key, extent, spread, limit, split=(), dtype=jnp.bfloat16):
    result = jax.random.normal(own_key, extent, jnp.float32) * spread
    if len(split) > 0:
        result = shard_levels(own_key, extent, split, -0.22, 0.18) * result
    return jnp.clip(result, min=-limit, max=limit).astype(dtype)


def bell_draw_with(stream_key, extent, deviation, most, cuts, heavy, held_as=jnp.bfloat16):
    result = deviation * jax.random.normal(stream_key, extent, jnp.float32)
    if cuts:
        result = result * shard_levels(stream_key, extent, cuts, -0.22, 0.18)
    return jnp.clip(spiked(result, jax.random.fold_in(stream_key, 3), *heavy), -most, most).astype(held_as)


def setup_inputs(seed: int = 0) -> dict:
    seeds = jax.random.split(jax.random.key(seed), 8)
    return {
        "anchor": gaussian(seeds[0], (D, D), D ** -0.5, 0.15625, ((0, 8), (1, 4)), jnp.float32),
        "momentum": gaussian(seeds[1], (D, D), 0.05, 0.75, ((0, 8), (1, 4)), jnp.float32),
        "change": gaussian(seeds[2], (REPLICAS, D, D), 0.05, 0.75, ((0, 4), (1, 8)), jnp.float32),
        "adam_first": gaussian(seeds[3], (REPLICAS, D, D), 0.3, 4.0, ((0, 4), (1, 8)), jnp.float32),
        "adam_second": jnp.clip(jnp.exp(math.log(2.0) - 2.9957323 * jax.random.uniform(seeds[4], (REPLICAS, D, D), jnp.float32) ** shard_levels(seeds[4], (REPLICAS, D, D), ((0, 4), (1, 8)), -0.2, 0.2)), 0.1, 2.0),
        "attn_out": bell_draw_with(seeds[5], (REPLICAS, TOKENS, D), 1.0, 6.0, ((0, 4), (1, 8)), (1, 2, 8, 2.0)),
        "grad_out": gaussian(seeds[6], (REPLICAS, TOKENS, D), 1.0, 6.0, ((0, 4), (1, 8))),
    }


outer_rate = 0.7
outer_mu = 0.9
inner_rate = 0.005
beta_one = 0.9
beta_two = 0.95
decay_rate = 0.1
epsilon = 1e-08

def reference(anchor, momentum, change, adam_first, adam_second, attn_out, grad_out):
    outer_grad = -lax.optimization_barrier(jnp.sum(change, axis=0)) / REPLICAS
    new_momentum = outer_mu * momentum + outer_grad
    new_anchor = anchor - outer_rate * (outer_grad + outer_mu * new_momentum)
    weights = new_anchor.astype(jnp.bfloat16)
    grad_scale = TOKENS ** (-0.5)

    def one_group(operands):
        inputs, cotangent, first, second = operands
        gradient = jnp.dot(inputs.T, cotangent, preferred_element_type=jnp.float32) * grad_scale
        first_next = beta_one * first + (1.0 - beta_one) * gradient
        second_next = beta_two * second + (1.0 - beta_two) * gradient * gradient
        local = new_anchor - inner_rate * (first_next / (jnp.sqrt(second_next) + epsilon) + decay_rate * new_anchor)
        back = jnp.dot(cotangent, weights.T, preferred_element_type=jnp.float32).astype(jnp.bfloat16)
        return (local, first_next, second_next, back)
    results = lax.map(one_group, (attn_out, grad_out, adam_first, adam_second))
    return (new_anchor, new_momentum, results[0], results[1], results[2], results[3])
```

```python
import functools

import jax
import jax.numpy as jnp
from jax import lax
from jax.experimental import pallas as pl
from jax.experimental.pallas import tpu as pltpu
from jax.sharding import PartitionSpec as P

outer_rate = 0.7
outer_mu = 0.9
inner_rate = 0.005
beta_one = 0.9
beta_two = 0.95
decay_rate = 0.1
epsilon = 1e-08

MESH = pl.DeviceIdType.MESH
f32 = jnp.float32
bf16 = jnp.bfloat16


def adam(anchor_next, first, second, gradient):
    first_next = beta_one * first + (1.0 - beta_one) * gradient
    second_next = beta_two * second + (1.0 - beta_two) * gradient * gradient
    local = anchor_next - inner_rate * (
        first_next / (jnp.sqrt(second_next) + epsilon) + decay_rate * anchor_next
    )
    return local, first_next, second_next


def outer_step(anchor, momentum, summed, groups):
    outer_grad = -summed / groups
    new_momentum = outer_mu * momentum + outer_grad
    new_anchor = anchor - outer_rate * (outer_grad + outer_mu * new_momentum)
    return new_anchor, new_momentum


def plain_shards(anchor, momentum, change, adam_first, adam_second, attn_out, grad_out):
    groups = lax.axis_size("replica")
    summed = lax.psum_scatter(change[0], "replica", scatter_dimension=1, tiled=True)
    new_anchor, new_momentum = outer_step(anchor, momentum, summed, groups)
    anchor_next = lax.all_gather(new_anchor, "replica", axis=1, tiled=True)
    inputs, cotangent = attn_out[0], grad_out[0]
    grad_scale = (inputs.shape[0] * lax.axis_size("fsdp")) ** (-0.5)
    gradient = grad_scale * lax.psum_scatter(
        lax.dot_general(inputs, cotangent, (((0,), (0,)), ((), ())), preferred_element_type=f32),
        "fsdp",
        scatter_dimension=0,
        tiled=True,
    )
    input_grad = lax.dot_general(
        cotangent,
        lax.all_gather(anchor_next.astype(bf16), "fsdp", axis=0, tiled=True),
        (((1,), (1,)), ((), ())),
        preferred_element_type=f32,
    ).astype(bf16)
    local, first, second = adam(anchor_next, adam_first[0], adam_second[0], gradient)
    return new_anchor, new_momentum, local[None], first[None], second[None], input_grad[None]


def kernel(
    depth, groups, scale,
    anchor_hbm, momentum_hbm, change_hbm, attn_hbm, cot_hbm,
    summed_ref, row_ref, grad_ref, back_hbm,
    anchor, momentum, change, attn, cot, flipped,
    part, got, own, psend, ry, zsend, chain, weights, back,
    local_sem, back_sem, part_s, part_r, py_s, py_r, ch_s, ch_r,
    az_s, az_r, ay_s, ay_r, ax_s, ax_r, as_s, as_r,
):
    r = lax.axis_index("replica")
    f = lax.axis_index("fsdp")
    x, core = r // 2, r % 2
    z, y = f // 2, f % 2
    rows, width = change.shape
    cols = width // groups
    pair = 2 * rows
    flip_y = {"replica": r, "fsdp": z * 2 + (1 - y)}
    flip_x = {"replica": (1 - x) * 2 + core, "fsdp": f}
    sibling = {"replica": x * 2 + (1 - core), "fsdp": f}

    def along_z(where):
        return {"replica": r, "fsdp": where * 2 + y}

    loads = []
    for i, (src, dst) in enumerate((
        (change_hbm, change), (anchor_hbm, anchor), (momentum_hbm, momentum),
        (attn_hbm, attn), (cot_hbm, cot),
    )):
        loads.append(pltpu.make_async_copy(src, dst, local_sem.at[i]))
        loads[-1].start()

    barrier = pltpu.get_barrier_semaphore()
    for k in range(1, groups):
        pl.semaphore_signal(
            barrier, inc=1, device_id={"replica": (r + k) % groups, "fsdp": f}, device_id_type=MESH
        )
    for k in range(1, depth):
        pl.semaphore_signal(barrier, inc=1, device_id=along_z((z + k) % depth), device_id_type=MESH)
    pl.semaphore_signal(barrier, inc=1, device_id=flip_y, device_id_type=MESH)

    def remote(src, dst, send, recv, device):
        return pltpu.make_async_remote_copy(
            src_ref=src, dst_ref=dst, send_sem=send, recv_sem=recv,
            device_id=device, device_id_type=MESH,
        )

    loads[0].wait()
    for k in range(groups):
        at = pl.multiple_of(((r + k) % groups) * cols, 128)
        part[k] = change[:, pl.ds(at, cols)].astype(bf16)
    pl.semaphore_wait(barrier, groups + depth - 1)
    parts = []
    for k in range(1, groups):
        parts.append(remote(
            part.at[k], got.at[k - 1], part_s.at[k - 1], part_r.at[k - 1],
            {"replica": (r + k) % groups, "fsdp": f},
        ))
        parts[-1].start()

    def block_at(i):
        low = jnp.where(i < depth - 1 - z, depth - 1 - i, i - (depth - 1 - z))
        high = jnp.where(i < z, i, depth - 1 - (i - z))
        return jnp.where(z < depth // 2, low, high)

    loads[3].wait()
    loads[4].wait()
    tile = 512 if width % 512 == 0 else 128
    y_copies = [
        remote(psend.at[i], ry.at[i], py_s.at[i], py_r.at[i], flip_y) for i in range(depth)
    ]

    def multiply(i):
        at = pl.multiple_of(block_at(i) * pair, 128)
        flipped[...] = attn[:, pl.ds(at, pair)].T

        def columns(c, carry):
            there = pl.ds(pl.multiple_of(c * tile, 128), tile)
            product = jnp.dot(flipped[...], cot[:, there], preferred_element_type=f32)
            upper, lower = product[:rows], product[rows:]
            own[i, :, there] = jnp.where(y == 0, upper, lower)
            psend[i, :, there] = jnp.where(y == 0, lower, upper).astype(bf16)
            return carry

        lax.fori_loop(0, width // tile, columns, 0)

    for i in range(depth):
        multiply(i)
        if i < 2:
            y_copies[i].start()

    loads[1].wait()
    loads[2].wait()
    for k in range(1, groups):
        parts[k - 1].wait_recv()
    mine = pl.ds(pl.multiple_of(r * cols, 128), cols)
    total = change[:, mine]
    for k in range(1, groups):
        total = total + got[k - 1].astype(f32)
    summed_ref[...] = total
    weights[f, :, mine] = outer_step(anchor[...], momentum[...], total, groups)[0].astype(bf16)

    def shard(zs, ys, xs, cs):
        at = pl.multiple_of((xs * 2 + cs) * cols, 128)
        return weights.at[zs * 2 + ys, :, pl.ds(at, cols)]

    def forward(kind, sends, recvs, index, where, device):
        ref = shard(*where)
        copy = remote(ref, ref, sends.at[index], recvs.at[index], device)
        copy.start()
        return copy

    def arrived(recvs, sends, index, where):
        ref = shard(*where)
        remote(ref, ref, sends.at[index], recvs.at[index], sibling).wait_recv()

    pending = []
    here = (z, y, x, core)
    for k in range(1, depth):
        pending.append(forward("z", az_s, az_r, k - 1, here, along_z((z + k) % depth)))
    pending.append(forward("y", ay_s, ay_r, 0, here, flip_y))
    pending.append(forward("x", ax_s, ax_r, 0, here, flip_x))
    pending.append(forward("s", as_s, as_r, 0, here, sibling))
    for k in range(1, depth):
        where = ((z + depth - k) % depth, y, x, core)
        arrived(az_r, az_s, k - 1, where)
        pending.append(forward("y", ay_s, ay_r, k, where, flip_y))
        pending.append(forward("x", ax_s, ax_r, k, where, flip_x))
        pending.append(forward("s", as_s, as_r, k, where, sibling))
    for i in range(2, depth):
        y_copies[i].start()

    lines = 16

    def reduce_step(i):
        y_copies[i].wait_recv()
        dest = block_at(i)
        up = dest > z
        slot = dest + jnp.where(up, 0, depth)
        follows = jnp.where(up, z > 0, z < depth - 1)
        copy = remote(
            zsend.at[i], chain.at[slot], ch_s.at[i], ch_r.at[slot],
            along_z(z + jnp.where(up, 1, -1)),
        )

        @pl.when(follows)
        def _():
            copy.wait_recv()

            def add(j, carry):
                there = pl.ds(pl.multiple_of(j * lines, lines), lines)
                zsend[i, there] = (
                    own[i, there] + ry[i, there].astype(f32) + chain[slot, there].astype(f32)
                ).astype(bf16)
                return carry

            lax.fori_loop(0, rows // lines, add, 0)

        @pl.when(jnp.logical_not(follows))
        def _():
            def add(j, carry):
                there = pl.ds(pl.multiple_of(j * lines, lines), lines)
                zsend[i, there] = (own[i, there] + ry[i, there].astype(f32)).astype(bf16)
                return carry

            lax.fori_loop(0, rows // lines, add, 0)

        copy.start()
        return copy

    chains = [reduce_step(0)]
    for k in range(depth):
        where = ((z + depth - k) % depth, 1 - y, x, core)
        arrived(ay_r, ay_s, k, where)
        pending.append(forward("x", ax_s, ax_r, depth + k, where, flip_x))
        pending.append(forward("s", as_s, as_r, depth + k, where, sibling))
    for i in range(1, depth - 1):
        chains.append(reduce_step(i))
    for dy in range(2):
        for k in range(depth):
            where = ((z + depth - k) % depth, y + dy - 2 * y * dy, 1 - x, core)
            arrived(ax_r, ax_s, dy * depth + k, where)
            pending.append(forward("s", as_s, as_r, (2 + dy) * depth + k, where, sibling))
    for dx in range(2):
        for dy in range(2):
            for k in range(depth):
                where = (
                    (z + depth - k) % depth, y + dy - 2 * y * dy, x + dx - 2 * x * dx, 1 - core
                )
                arrived(as_r, as_s, (2 * dx + dy) * depth + k, where)
    row_ref[...] = weights[f]

    def back_copy(c):
        there = pl.ds(pl.multiple_of(c * pair, 128), pair)
        return pltpu.make_async_copy(back.at[:, there], back_hbm.at[:, there], back_sem.at[c])

    def back_step(c, carry):
        there = pl.ds(pl.multiple_of(c * pair, 128), pair)
        block = weights[pl.ds(2 * c, 2)].reshape(pair, width)
        back[:, there] = lax.dot_general(
            cot[...], block, (((1,), (1,)), ((), ())), preferred_element_type=f32
        ).astype(bf16)
        return carry

    for c in range(depth):
        back_step(c, 0)
        back_copy(c).start()

    last = depth - 1
    y_copies[last].wait_recv()
    grad_ref[...] = (own[last] + ry[last].astype(f32)) * scale
    for slot, follows in ((z, z > 0), (depth + z, z < depth - 1)):
        @pl.when(follows)
        def _():
            remote(
                zsend.at[0], chain.at[slot], ch_s.at[0], ch_r.at[slot], flip_y
            ).wait_recv()
            grad_ref[...] += chain[slot].astype(f32) * scale

    for copy in parts + y_copies + pending + chains:
        copy.wait_send()
    for c in range(depth):
        back_copy(c).wait()


def fused_shards(anchor, momentum, change, adam_first, adam_second, attn_out, grad_out):
    groups, devices = lax.axis_size("replica"), lax.axis_size("fsdp")
    depth = devices // 2
    rows, width = change.shape[1:]
    tokens = attn_out.shape[1]
    cols = width // groups
    scale = (tokens * devices) ** (-0.5)
    dma = pltpu.SemaphoreType.DMA
    vmem = pltpu.VMEM
    any_space = pl.BlockSpec(memory_space=pl.ANY)
    in_vmem = pl.BlockSpec(memory_space=pltpu.VMEM)
    summed, anchor_row, gradient, input_grad = pl.pallas_call(
        functools.partial(kernel, depth, groups, scale),
        out_shape=(
            jax.ShapeDtypeStruct((rows, cols), f32),
            jax.ShapeDtypeStruct((rows, width), bf16),
            jax.ShapeDtypeStruct((rows, width), f32),
            jax.ShapeDtypeStruct((tokens, width), bf16),
        ),
        in_specs=[any_space] * 5,
        out_specs=(in_vmem, in_vmem, in_vmem, any_space),
        scratch_shapes=[
            vmem((rows, cols), f32),
            vmem((rows, cols), f32),
            vmem((rows, width), f32),
            vmem((tokens, width), bf16),
            vmem((tokens, width), bf16),
            vmem((2 * rows, tokens), bf16),
            vmem((groups, rows, cols), bf16),
            vmem((groups - 1, rows, cols), bf16),
            vmem((depth, rows, width), f32),
            vmem((depth, rows, width), bf16),
            vmem((depth, rows, width), bf16),
            vmem((depth, rows, width), bf16),
            vmem((2 * depth, rows, width), bf16),
            vmem((devices, rows, width), bf16),
            vmem((tokens, width), bf16),
            dma((5,)), dma((depth,)),
            dma((groups - 1,)), dma((groups - 1,)),
            dma((depth,)), dma((depth,)),
            dma((depth,)), dma((2 * depth,)),
            dma((depth - 1,)), dma((depth - 1,)),
            dma((depth,)), dma((depth,)),
            dma((2 * depth,)), dma((2 * depth,)),
            dma((4 * depth,)), dma((4 * depth,)),
        ],
        compiler_params=pltpu.CompilerParams(
            collective_id=0, has_side_effects=True, vmem_limit_bytes=60 * 2**20
        ),
    )(anchor, momentum, change[0], attn_out[0], grad_out[0])
    new_anchor, new_momentum = outer_step(anchor, momentum, summed, groups)
    local, first, second = adam(anchor_row.astype(f32), adam_first[0], adam_second[0], gradient)
    return new_anchor, new_momentum, local[None], first[None], second[None], input_grad[None]


def shards(*arrays):
    groups, devices = lax.axis_size("replica"), lax.axis_size("fsdp")
    rows, width = arrays[2].shape[1:]
    fits = (
        groups == 4 and devices % 2 == 0 and devices >= 4 and rows % 32 == 0
        and (2 * rows) % 128 == 0 and width % (128 * groups) == 0
        and arrays[5].shape[1] * width <= 2**21
    )
    return (fused_shards if fits else plain_shards)(*arrays)


def solution(mesh):
    in_specs = (P("fsdp", "replica"),) * 2 + (P("replica", "fsdp", None),) * 5
    out_specs = (P("fsdp", "replica"),) * 2 + (P("replica", "fsdp", None),) * 4
    return jax.shard_map(shards, mesh=mesh, in_specs=in_specs, out_specs=out_specs, check_vma=False)
```

```python
import functools

import jax
import jax.numpy as jnp
from jax import lax
from jax.experimental import pallas as pl
from jax.experimental.pallas import tpu as pltpu
from jax.sharding import PartitionSpec as P

outer_rate = 0.7
outer_mu = 0.9
inner_rate = 0.005
beta_one = 0.9
beta_two = 0.95
decay_rate = 0.1
epsilon = 1e-08

MESH = pl.DeviceIdType.MESH
f32 = jnp.float32
bf16 = jnp.bfloat16


def adam(anchor_next, first, second, gradient):
    first_next = beta_one * first + (1.0 - beta_one) * gradient
    second_next = beta_two * second + (1.0 - beta_two) * gradient * gradient
    local = anchor_next - inner_rate * (
        first_next / (jnp.sqrt(second_next) + epsilon) + decay_rate * anchor_next
    )
    return local, first_next, second_next


def outer_step(anchor, momentum, summed, groups):
    outer_grad = -summed / groups
    new_momentum = outer_mu * momentum + outer_grad
    new_anchor = anchor - outer_rate * (outer_grad + outer_mu * new_momentum)
    return new_anchor, new_momentum


def plain_shards(anchor, momentum, change, adam_first, adam_second, attn_out, grad_out):
    groups = lax.axis_size("replica")
    summed = lax.psum_scatter(change[0], "replica", scatter_dimension=1, tiled=True)
    new_anchor, new_momentum = outer_step(anchor, momentum, summed, groups)
    anchor_next = lax.all_gather(new_anchor, "replica", axis=1, tiled=True)
    inputs, cotangent = attn_out[0], grad_out[0]
    grad_scale = (inputs.shape[0] * lax.axis_size("fsdp")) ** (-0.5)
    gradient = grad_scale * lax.psum_scatter(
        lax.dot_general(inputs, cotangent, (((0,), (0,)), ((), ())), preferred_element_type=f32),
        "fsdp",
        scatter_dimension=0,
        tiled=True,
    )
    input_grad = lax.dot_general(
        cotangent,
        lax.all_gather(anchor_next.astype(bf16), "fsdp", axis=0, tiled=True),
        (((1,), (1,)), ((), ())),
        preferred_element_type=f32,
    ).astype(bf16)
    local, first, second = adam(anchor_next, adam_first[0], adam_second[0], gradient)
    return new_anchor, new_momentum, local[None], first[None], second[None], input_grad[None]


def kernel(
    depth, groups, scale,
    anchor_hbm, momentum_hbm, change_hbm, attn_hbm, cot_hbm,
    summed_ref, row_ref, grad_ref, back_hbm,
    anchor, momentum, change, attn, cot, flipped,
    part, got, own, psend, ry, zsend, chain, weights, back,
    lead_own, lead_send, lead_chain, lead_out, lead_in,
    local_sem, back_sem, part_s, part_r, py_s, py_r, ch_s, ch_r,
    lz_s, lz_r, ly_s, ly_r,
    az_s, az_r, ay_s, ay_r, ax_s, ax_r, as_s, as_r,
):
    r = lax.axis_index("replica")
    f = lax.axis_index("fsdp")
    x, core = r // 2, r % 2
    z, y = f // 2, f % 2
    rows, width = change.shape
    cols = width // groups
    pair = 2 * rows
    flip_y = {"replica": r, "fsdp": z * 2 + (1 - y)}
    flip_x = {"replica": (1 - x) * 2 + core, "fsdp": f}
    sibling = {"replica": x * 2 + (1 - core), "fsdp": f}

    def along_z(where):
        return {"replica": r, "fsdp": where * 2 + y}

    loads = []
    for i, (src, dst) in enumerate((
        (change_hbm, change), (anchor_hbm, anchor), (momentum_hbm, momentum),
        (attn_hbm, attn), (cot_hbm, cot),
    )):
        loads.append(pltpu.make_async_copy(src, dst, local_sem.at[i]))
        loads[-1].start()

    barrier = pltpu.get_barrier_semaphore()
    for k in range(1, groups):
        pl.semaphore_signal(
            barrier, inc=1, device_id={"replica": (r + k) % groups, "fsdp": f}, device_id_type=MESH
        )
    for k in range(1, depth):
        pl.semaphore_signal(barrier, inc=1, device_id=along_z((z + k) % depth), device_id_type=MESH)
    pl.semaphore_signal(barrier, inc=1, device_id=flip_y, device_id_type=MESH)

    def remote(src, dst, send, recv, device):
        return pltpu.make_async_remote_copy(
            src_ref=src, dst_ref=dst, send_sem=send, recv_sem=recv,
            device_id=device, device_id_type=MESH,
        )

    loads[0].wait()
    for k in range(groups):
        at = pl.multiple_of(((r + k) % groups) * cols, 128)
        part[k] = change[:, pl.ds(at, cols)].astype(bf16)
    pl.semaphore_wait(barrier, groups + depth - 1)
    parts = []
    for k in range(1, groups):
        parts.append(remote(
            part.at[k], got.at[k - 1], part_s.at[k - 1], part_r.at[k - 1],
            {"replica": (r + k) % groups, "fsdp": f},
        ))
        parts[-1].start()

    def block_at(i):
        low = jnp.where(i < depth - 1 - z, depth - 1 - i, i - (depth - 1 - z))
        high = jnp.where(i < z, i, depth - 1 - (i - z))
        return jnp.where(z < depth // 2, low, high)

    lead = lead_own.shape[2]
    half = (width - lead) // 2
    last = depth - 1
    inner = jnp.logical_and(z > 0, z < last)

    def y_copy(i, h):
        there = pl.ds(pl.multiple_of(h * half, 128), half)
        return remote(
            psend.at[i, :, there], ry.at[i, :, there], py_s.at[2 * i + h], py_r.at[2 * i + h],
            flip_y,
        )

    def route(i):
        dest = block_at(i)
        up = dest > z
        return dest + jnp.where(up, 0, depth), along_z(z + jnp.where(up, 1, -1))

    def lead_copy(i):
        slot, device = route(i)
        return remote(
            lead_send.at[i], lead_chain.at[slot], lz_s.at[i], lz_r.at[slot], device
        )

    loads[3].wait()
    loads[4].wait()

    def multiply(i, carry):
        at = pl.multiple_of(block_at(i) * pair, 128)
        flipped[...] = attn[:, pl.ds(at, pair)].T

        def columns(h, carry):
            there = pl.ds(pl.multiple_of(lead + h * half, 128), half)
            product = jnp.dot(flipped[...], cot[:, there], preferred_element_type=f32)
            upper, lower = product[:rows], product[rows:]
            here = pl.ds(pl.multiple_of(h * half, 128), half)
            own[i, :, here] = jnp.where(y == 0, upper, lower)
            psend[i, :, here] = jnp.where(y == 0, lower, upper).astype(bf16)

            @pl.when(i < 2)
            def _():
                y_copy(i, h).start()

            return carry

        lax.fori_loop(0, 2, columns, 0)
        lead_own[i] = jnp.dot(flipped[...], cot[:, :lead], preferred_element_type=f32)

        @pl.when(jnp.logical_and(jnp.logical_not(inner), i < last))
        def _():
            lead_send[i] = lead_own[i].astype(bf16)
            lead_copy(i).start()

        return carry

    lax.fori_loop(0, depth, multiply, 0)

    loads[1].wait()
    loads[2].wait()
    for k in range(1, groups):
        parts[k - 1].wait_recv()
    mine = pl.ds(pl.multiple_of(r * cols, 128), cols)
    total = change[:, mine]
    for k in range(1, groups):
        total = total + got[k - 1].astype(f32)
    summed_ref[...] = total
    weights[f, :, mine] = outer_step(anchor[...], momentum[...], total, groups)[0].astype(bf16)

    def shard(zs, ys, xs, cs):
        at = pl.multiple_of((xs * 2 + cs) * cols, 128)
        return weights.at[zs * 2 + ys, :, pl.ds(at, cols)]

    def forward(kind, sends, recvs, index, where, device):
        ref = shard(*where)
        copy = remote(ref, ref, sends.at[index], recvs.at[index], device)
        copy.start()
        return copy

    def arrived(recvs, sends, index, where):
        ref = shard(*where)
        remote(ref, ref, sends.at[index], recvs.at[index], sibling).wait_recv()

    pending = []
    here = (z, y, x, core)
    for k in range(1, depth):
        pending.append(forward("z", az_s, az_r, k - 1, here, along_z((z + k) % depth)))
    pending.append(forward("y", ay_s, ay_r, 0, here, flip_y))
    pending.append(forward("x", ax_s, ax_r, 0, here, flip_x))
    pending.append(forward("s", as_s, as_r, 0, here, sibling))

    @pl.when(inner)
    def _():
        def pass_on(i, carry):
            slot, _ = route(i)
            copy = lead_copy(i)
            copy.wait_recv()
            lead_send[i] = (lead_own[i] + lead_chain[slot].astype(f32)).astype(bf16)
            copy.start()
            return carry

        lax.fori_loop(0, last, pass_on, 0)

    for k in range(1, depth):
        where = ((z + depth - k) % depth, y, x, core)
        arrived(az_r, az_s, k - 1, where)
        pending.append(forward("y", ay_s, ay_r, k, where, flip_y))
        pending.append(forward("x", ax_s, ax_r, k, where, flip_x))
        pending.append(forward("s", as_s, as_r, k, where, sibling))
    for i in range(2, depth):
        for h in range(2):
            y_copy(i, h).start()

    lines = 16

    def reduce_step(i):
        for h in range(2):
            y_copy(i, h).wait_recv()
        slot, device = route(i)
        copy = remote(zsend.at[i], chain.at[slot], ch_s.at[i], ch_r.at[slot], device)

        @pl.when(inner)
        def _():
            copy.wait_recv()

            def add(j, carry):
                there = pl.ds(pl.multiple_of(j * lines, lines), lines)
                zsend[i, there] = (
                    own[i, there] + ry[i, there].astype(f32) + chain[slot, there].astype(f32)
                ).astype(bf16)
                return carry

            lax.fori_loop(0, rows // lines, add, 0)

        @pl.when(jnp.logical_not(inner))
        def _():
            def add(j, carry):
                there = pl.ds(pl.multiple_of(j * lines, lines), lines)
                zsend[i, there] = (own[i, there] + ry[i, there].astype(f32)).astype(bf16)
                return carry

            lax.fori_loop(0, rows // lines, add, 0)

        copy.start()
        return copy

    chains = [reduce_step(0)]
    for k in range(depth):
        where = ((z + depth - k) % depth, 1 - y, x, core)
        arrived(ay_r, ay_s, k, where)
        pending.append(forward("x", ax_s, ax_r, depth + k, where, flip_x))
        pending.append(forward("s", as_s, as_r, depth + k, where, sibling))
    for slot, follows in ((z, z > 0), (depth + z, z < last)):
        @pl.when(follows)
        def _():
            remote(
                lead_send.at[0], lead_chain.at[slot], lz_s.at[0], lz_r.at[slot], flip_y
            ).wait_recv()
            lead_own[last] += lead_chain[slot].astype(f32)
    lead_out[...] = lead_own[last, pl.ds(pl.multiple_of((1 - y) * rows, 8), rows)].astype(bf16)
    lead_swap = remote(lead_out, lead_in, ly_s.at[0], ly_r.at[0], flip_y)
    lead_swap.start()
    for i in range(1, last):
        chains.append(reduce_step(i))
    for dy in range(2):
        for k in range(depth):
            where = ((z + depth - k) % depth, y + dy - 2 * y * dy, 1 - x, core)
            arrived(ax_r, ax_s, dy * depth + k, where)
            pending.append(forward("s", as_s, as_r, (2 + dy) * depth + k, where, sibling))
    for dx in range(2):
        for dy in range(2):
            for k in range(depth):
                where = (
                    (z + depth - k) % depth, y + dy - 2 * y * dy, x + dx - 2 * x * dx, 1 - core
                )
                arrived(as_r, as_s, (2 * dx + dy) * depth + k, where)
    row_ref[...] = weights[f]

    def back_copy(c):
        there = pl.ds(pl.multiple_of(c * pair, 128), pair)
        return pltpu.make_async_copy(back.at[:, there], back_hbm.at[:, there], back_sem.at[c])

    def back_step(c, carry):
        there = pl.ds(pl.multiple_of(c * pair, 128), pair)
        block = weights[pl.ds(2 * c, 2)].reshape(pair, width)
        back[:, there] = lax.dot_general(
            cot[...], block, (((1,), (1,)), ((), ())), preferred_element_type=f32
        ).astype(bf16)
        back_copy(c).start()
        return carry

    lax.fori_loop(0, depth, back_step, 0)

    lead_swap.wait_recv()
    kept = lead_own[last, pl.ds(pl.multiple_of(y * rows, 8), rows)]
    grad_ref[:, :lead] = (kept + lead_in[...].astype(f32)) * scale
    for h in range(2):
        y_copy(last, h).wait_recv()
    grad_ref[:, lead:] = (own[last] + ry[last].astype(f32)) * scale
    for slot, follows in ((z, z > 0), (depth + z, z < last)):
        @pl.when(follows)
        def _():
            remote(
                zsend.at[0], chain.at[slot], ch_s.at[0], ch_r.at[slot], flip_y
            ).wait_recv()
            grad_ref[:, lead:] += chain[slot].astype(f32) * scale

    for copy in parts + pending + chains + [lead_swap]:
        copy.wait_send()
    for i in range(depth):
        for h in range(2):
            y_copy(i, h).wait_send()
    for i in range(last):
        lead_copy(i).wait_send()
    for c in range(depth):
        back_copy(c).wait()


def lead_columns(width):
    return width // 6 // 128 * 128


def fused_shards(anchor, momentum, change, adam_first, adam_second, attn_out, grad_out):
    groups, devices = lax.axis_size("replica"), lax.axis_size("fsdp")
    depth = devices // 2
    rows, width = change.shape[1:]
    tokens = attn_out.shape[1]
    cols = width // groups
    lead = lead_columns(width)
    rest = width - lead
    scale = (tokens * devices) ** (-0.5)
    dma = pltpu.SemaphoreType.DMA
    vmem = pltpu.VMEM
    any_space = pl.BlockSpec(memory_space=pl.ANY)
    in_vmem = pl.BlockSpec(memory_space=pltpu.VMEM)
    summed, anchor_row, gradient, input_grad = pl.pallas_call(
        functools.partial(kernel, depth, groups, scale),
        out_shape=(
            jax.ShapeDtypeStruct((rows, cols), f32),
            jax.ShapeDtypeStruct((rows, width), bf16),
            jax.ShapeDtypeStruct((rows, width), f32),
            jax.ShapeDtypeStruct((tokens, width), bf16),
        ),
        in_specs=[any_space] * 5,
        out_specs=(in_vmem, in_vmem, in_vmem, any_space),
        scratch_shapes=[
            vmem((rows, cols), f32),
            vmem((rows, cols), f32),
            vmem((rows, width), f32),
            vmem((tokens, width), bf16),
            vmem((tokens, width), bf16),
            vmem((2 * rows, tokens), bf16),
            vmem((groups, rows, cols), bf16),
            vmem((groups - 1, rows, cols), bf16),
            vmem((depth, rows, rest), f32),
            vmem((depth, rows, rest), bf16),
            vmem((depth, rows, rest), bf16),
            vmem((depth, rows, rest), bf16),
            vmem((2 * depth, rows, rest), bf16),
            vmem((devices, rows, width), bf16),
            vmem((tokens, width), bf16),
            vmem((depth, 2 * rows, lead), f32),
            vmem((depth, 2 * rows, lead), bf16),
            vmem((2 * depth, 2 * rows, lead), bf16),
            vmem((rows, lead), bf16),
            vmem((rows, lead), bf16),
            dma((5,)), dma((depth,)),
            dma((groups - 1,)), dma((groups - 1,)),
            dma((2 * depth,)), dma((2 * depth,)),
            dma((depth,)), dma((2 * depth,)),
            dma((depth,)), dma((2 * depth,)), dma((1,)), dma((1,)),
            dma((depth - 1,)), dma((depth - 1,)),
            dma((depth,)), dma((depth,)),
            dma((2 * depth,)), dma((2 * depth,)),
            dma((4 * depth,)), dma((4 * depth,)),
        ],
        compiler_params=pltpu.CompilerParams(
            collective_id=0, has_side_effects=True, vmem_limit_bytes=60 * 2**20
        ),
    )(anchor, momentum, change[0], attn_out[0], grad_out[0])
    new_anchor, new_momentum = outer_step(anchor, momentum, summed, groups)
    local, first, second = adam(anchor_row.astype(f32), adam_first[0], adam_second[0], gradient)
    return new_anchor, new_momentum, local[None], first[None], second[None], input_grad[None]


def shards(*arrays):
    groups, devices = lax.axis_size("replica"), lax.axis_size("fsdp")
    rows, width = arrays[2].shape[1:]
    fits = (
        groups == 4 and devices % 2 == 0 and devices >= 4 and rows % 32 == 0
        and (2 * rows) % 128 == 0 and width % (128 * groups) == 0
        and lead_columns(width) > 0 and (width - lead_columns(width)) % 256 == 0
        and arrays[5].shape[1] * width <= 2**21
    )
    return (fused_shards if fits else plain_shards)(*arrays)


def solution(mesh):
    in_specs = (P("fsdp", "replica"),) * 2 + (P("replica", "fsdp", None),) * 5
    out_specs = (P("fsdp", "replica"),) * 2 + (P("replica", "fsdp", None),) * 4
    return jax.shard_map(shards, mesh=mesh, in_specs=in_specs, out_specs=out_specs, check_vma=False)
```

```python
import functools

import jax
import jax.numpy as jnp
from jax import lax
from jax.experimental import pallas as pl
from jax.experimental.pallas import tpu as pltpu
from jax.sharding import PartitionSpec as P

outer_rate = 0.7
outer_mu = 0.9
inner_rate = 0.005
beta_one = 0.9
beta_two = 0.95
decay_rate = 0.1
epsilon = 1e-08

MESH = pl.DeviceIdType.MESH
f32 = jnp.float32
bf16 = jnp.bfloat16


def adam(anchor_next, first, second, gradient):
    first_next = beta_one * first + (1.0 - beta_one) * gradient
    second_next = beta_two * second + (1.0 - beta_two) * gradient * gradient
    local = anchor_next - inner_rate * (
        first_next / (jnp.sqrt(second_next) + epsilon) + decay_rate * anchor_next
    )
    return local, first_next, second_next


def outer_step(anchor, momentum, summed, groups):
    outer_grad = -summed / groups
    new_momentum = outer_mu * momentum + outer_grad
    new_anchor = anchor - outer_rate * (outer_grad + outer_mu * new_momentum)
    return new_anchor, new_momentum


def plain_shards(anchor, momentum, change, adam_first, adam_second, attn_out, grad_out):
    groups = lax.axis_size("replica")
    summed = lax.psum_scatter(change[0], "replica", scatter_dimension=1, tiled=True)
    new_anchor, new_momentum = outer_step(anchor, momentum, summed, groups)
    anchor_next = lax.all_gather(new_anchor, "replica", axis=1, tiled=True)
    inputs, cotangent = attn_out[0], grad_out[0]
    grad_scale = (inputs.shape[0] * lax.axis_size("fsdp")) ** (-0.5)
    gradient = grad_scale * lax.psum_scatter(
        lax.dot_general(inputs, cotangent, (((0,), (0,)), ((), ())), preferred_element_type=f32),
        "fsdp",
        scatter_dimension=0,
        tiled=True,
    )
    input_grad = lax.dot_general(
        cotangent,
        lax.all_gather(anchor_next.astype(bf16), "fsdp", axis=0, tiled=True),
        (((1,), (1,)), ((), ())),
        preferred_element_type=f32,
    ).astype(bf16)
    local, first, second = adam(anchor_next, adam_first[0], adam_second[0], gradient)
    return new_anchor, new_momentum, local[None], first[None], second[None], input_grad[None]


def kernel(
    depth, groups, scale,
    anchor_hbm, momentum_hbm, change_hbm, attn_hbm, cot_hbm,
    summed_ref, row_ref, grad_ref, back_hbm,
    anchor, momentum, change, attn, cot, flipped,
    part, got, own, psend, ry, zsend, chain, weights, back,
    lead_own, lead_send, lead_chain, lead_out, lead_in,
    local_sem, back_sem, part_s, part_r, py_s, py_r, ch_s, ch_r,
    lz_s, lz_r, ly_s, ly_r,
    az_s, az_r, ay_s, ay_r, ax_s, ax_r, as_s, as_r,
):
    r = lax.axis_index("replica")
    f = lax.axis_index("fsdp")
    x, core = r // 2, r % 2
    z, y = f // 2, f % 2
    rows, width = change.shape
    cols = width // groups
    pair = 2 * rows
    flip_y = {"replica": r, "fsdp": z * 2 + (1 - y)}
    flip_x = {"replica": (1 - x) * 2 + core, "fsdp": f}
    sibling = {"replica": x * 2 + (1 - core), "fsdp": f}

    def along_z(where):
        return {"replica": r, "fsdp": where * 2 + y}

    loads = []
    for i, (src, dst) in enumerate((
        (change_hbm, change), (anchor_hbm, anchor), (momentum_hbm, momentum),
        (attn_hbm, attn), (cot_hbm, cot),
    )):
        loads.append(pltpu.make_async_copy(src, dst, local_sem.at[i]))
        loads[-1].start()

    barrier = pltpu.get_barrier_semaphore()
    for k in range(1, groups):
        pl.semaphore_signal(
            barrier, inc=1, device_id={"replica": (r + k) % groups, "fsdp": f}, device_id_type=MESH
        )
    for k in range(1, depth):
        pl.semaphore_signal(barrier, inc=1, device_id=along_z((z + k) % depth), device_id_type=MESH)
    pl.semaphore_signal(barrier, inc=1, device_id=flip_y, device_id_type=MESH)

    def remote(src, dst, send, recv, device):
        return pltpu.make_async_remote_copy(
            src_ref=src, dst_ref=dst, send_sem=send, recv_sem=recv,
            device_id=device, device_id_type=MESH,
        )

    loads[0].wait()
    for k in range(groups):
        at = pl.multiple_of(((r + k) % groups) * cols, 128)
        part[k] = change[:, pl.ds(at, cols)].astype(bf16)
    pl.semaphore_wait(barrier, groups + depth - 1)
    parts = []
    for k in range(1, groups):
        parts.append(remote(
            part.at[k], got.at[k - 1], part_s.at[k - 1], part_r.at[k - 1],
            {"replica": (r + k) % groups, "fsdp": f},
        ))
        parts[-1].start()

    def block_at(i):
        low = jnp.where(i < depth - 1 - z, depth - 1 - i, i - (depth - 1 - z))
        high = jnp.where(i < z, i, depth - 1 - (i - z))
        return jnp.where(z < depth // 2, low, high)

    lead = lead_own.shape[2]
    half = (width - lead) // 2
    last = depth - 1
    inner = jnp.logical_and(z > 0, z < last)

    def y_copy(i, h):
        there = pl.ds(pl.multiple_of(h * half, 128), half)
        return remote(
            psend.at[i, :, there], ry.at[i, :, there], py_s.at[2 * i + h], py_r.at[2 * i + h],
            flip_y,
        )

    def route(i):
        dest = block_at(i)
        up = dest > z
        return dest + jnp.where(up, 0, depth), along_z(z + jnp.where(up, 1, -1))

    def lead_copy(i):
        slot, device = route(i)
        return remote(
            lead_send.at[i], lead_chain.at[slot], lz_s.at[i], lz_r.at[slot], device
        )

    loads[3].wait()
    loads[4].wait()

    def multiply(i, carry):
        at = pl.multiple_of(block_at(i) * pair, 128)
        flipped[...] = attn[:, pl.ds(at, pair)].T

        def columns(h, carry):
            there = pl.ds(pl.multiple_of(lead + h * half, 128), half)
            product = jnp.dot(flipped[...], cot[:, there], preferred_element_type=f32)
            upper, lower = product[:rows], product[rows:]
            here = pl.ds(pl.multiple_of(h * half, 128), half)
            own[i, :, here] = jnp.where(y == 0, upper, lower)
            psend[i, :, here] = jnp.where(y == 0, lower, upper).astype(bf16)

            @pl.when(i < last)
            def _():
                y_copy(i, h).start()

            return carry

        lax.fori_loop(0, 2, columns, 0)
        lead_own[i] = jnp.dot(flipped[...], cot[:, :lead], preferred_element_type=f32)

        @pl.when(jnp.logical_and(jnp.logical_not(inner), i < last))
        def _():
            lead_send[i] = lead_own[i].astype(bf16)
            lead_copy(i).start()

        return carry

    lax.fori_loop(0, depth, multiply, 0)

    loads[1].wait()
    loads[2].wait()
    for k in range(1, groups):
        parts[k - 1].wait_recv()
    mine = pl.ds(pl.multiple_of(r * cols, 128), cols)
    total = change[:, mine]
    for k in range(1, groups):
        total = total + got[k - 1].astype(f32)
    summed_ref[...] = total
    weights[f, :, mine] = outer_step(anchor[...], momentum[...], total, groups)[0].astype(bf16)

    def shard(zs, ys, xs, cs):
        at = pl.multiple_of((xs * 2 + cs) * cols, 128)
        return weights.at[zs * 2 + ys, :, pl.ds(at, cols)]

    def forward(kind, sends, recvs, index, where, device):
        ref = shard(*where)
        copy = remote(ref, ref, sends.at[index], recvs.at[index], device)
        copy.start()
        return copy

    def arrived(recvs, sends, index, where):
        ref = shard(*where)
        remote(ref, ref, sends.at[index], recvs.at[index], sibling).wait_recv()

    pending = []
    here = (z, y, x, core)
    for k in range(1, depth):
        pending.append(forward("z", az_s, az_r, k - 1, here, along_z((z + k) % depth)))
    pending.append(forward("y", ay_s, ay_r, 0, here, flip_y))
    pending.append(forward("x", ax_s, ax_r, 0, here, flip_x))
    pending.append(forward("s", as_s, as_r, 0, here, sibling))

    lines = 16

    def chain_copy(i):
        slot, device = route(i)
        return remote(zsend.at[i], chain.at[slot], ch_s.at[i], ch_r.at[slot], device)

    def reduce_step(i, joins):
        for h in range(2):
            y_copy(i, h).wait_recv()
        copy = chain_copy(i)
        if joins:
            copy.wait_recv()
        slot, _ = route(i)

        def add(j, carry):
            there = pl.ds(pl.multiple_of(j * lines, lines), lines)
            total = own[i, there] + ry[i, there].astype(f32)
            if joins:
                total = total + chain[slot, there].astype(f32)
            zsend[i, there] = total.astype(bf16)
            return carry

        lax.fori_loop(0, rows // lines, add, 0)
        copy.start()

    outer = jnp.logical_not(inner)

    @pl.when(outer)
    def _():
        reduce_step(0, False)

    @pl.when(inner)
    def _():
        def pass_on(i, carry):
            slot, _ = route(i)
            copy = lead_copy(i)
            copy.wait_recv()
            lead_send[i] = (lead_own[i] + lead_chain[slot].astype(f32)).astype(bf16)
            copy.start()
            return carry

        lax.fori_loop(0, last, pass_on, 0)

    for k in range(1, depth):
        where = ((z + depth - k) % depth, y, x, core)
        arrived(az_r, az_s, k - 1, where)
        pending.append(forward("y", ay_s, ay_r, k, where, flip_y))
        pending.append(forward("x", ax_s, ax_r, k, where, flip_x))
        pending.append(forward("s", as_s, as_r, k, where, sibling))
    for h in range(2):
        y_copy(last, h).start()

    for slot, follows in ((z, z > 0), (depth + z, z < last)):
        @pl.when(follows)
        def _():
            remote(
                lead_send.at[0], lead_chain.at[slot], lz_s.at[0], lz_r.at[slot], flip_y
            ).wait_recv()
            lead_own[last] += lead_chain[slot].astype(f32)
    lead_out[...] = lead_own[last, pl.ds(pl.multiple_of((1 - y) * rows, 8), rows)].astype(bf16)
    lead_swap = remote(lead_out, lead_in, ly_s.at[0], ly_r.at[0], flip_y)
    lead_swap.start()

    @pl.when(outer)
    def _():
        for i in range(1, last):
            reduce_step(i, False)

    @pl.when(inner)
    def _():
        reduce_step(0, True)

    for k in range(depth):
        where = ((z + depth - k) % depth, 1 - y, x, core)
        arrived(ay_r, ay_s, k, where)
        pending.append(forward("x", ax_s, ax_r, depth + k, where, flip_x))
        pending.append(forward("s", as_s, as_r, depth + k, where, sibling))

    @pl.when(inner)
    def _():
        for i in range(1, last):
            reduce_step(i, True)

    for dy in range(2):
        for k in range(depth):
            where = ((z + depth - k) % depth, y + dy - 2 * y * dy, 1 - x, core)
            arrived(ax_r, ax_s, dy * depth + k, where)
            pending.append(forward("s", as_s, as_r, (2 + dy) * depth + k, where, sibling))
    for dx in range(2):
        for dy in range(2):
            for k in range(depth):
                where = (
                    (z + depth - k) % depth, y + dy - 2 * y * dy, x + dx - 2 * x * dx, 1 - core
                )
                arrived(as_r, as_s, (2 * dx + dy) * depth + k, where)
    row_ref[...] = weights[f]

    def back_copy(c):
        there = pl.ds(pl.multiple_of(c * pair, 128), pair)
        return pltpu.make_async_copy(back.at[:, there], back_hbm.at[:, there], back_sem.at[c])

    def back_step(c, carry):
        there = pl.ds(pl.multiple_of(c * pair, 128), pair)
        block = weights[pl.ds(2 * c, 2)].reshape(pair, width)
        back[:, there] = lax.dot_general(
            cot[...], block, (((1,), (1,)), ((), ())), preferred_element_type=f32
        ).astype(bf16)
        back_copy(c).start()
        return carry

    lax.fori_loop(0, depth, back_step, 0)

    lead_swap.wait_recv()
    kept = lead_own[last, pl.ds(pl.multiple_of(y * rows, 8), rows)]
    grad_ref[:, :lead] = (kept + lead_in[...].astype(f32)) * scale
    for h in range(2):
        y_copy(last, h).wait_recv()
    grad_ref[:, lead:] = (own[last] + ry[last].astype(f32)) * scale
    for slot, follows in ((z, z > 0), (depth + z, z < last)):
        @pl.when(follows)
        def _():
            remote(
                zsend.at[0], chain.at[slot], ch_s.at[0], ch_r.at[slot], flip_y
            ).wait_recv()
            grad_ref[:, lead:] += chain[slot].astype(f32) * scale

    for copy in parts + pending + [lead_swap]:
        copy.wait_send()
    for i in range(depth):
        for h in range(2):
            y_copy(i, h).wait_send()
    for i in range(last):
        lead_copy(i).wait_send()
        chain_copy(i).wait_send()
    for c in range(depth):
        back_copy(c).wait()


def lead_columns(width):
    return width // 6 // 128 * 128


def fused_shards(anchor, momentum, change, adam_first, adam_second, attn_out, grad_out):
    groups, devices = lax.axis_size("replica"), lax.axis_size("fsdp")
    depth = devices // 2
    rows, width = change.shape[1:]
    tokens = attn_out.shape[1]
    cols = width // groups
    lead = lead_columns(width)
    rest = width - lead
    scale = (tokens * devices) ** (-0.5)
    dma = pltpu.SemaphoreType.DMA
    vmem = pltpu.VMEM
    any_space = pl.BlockSpec(memory_space=pl.ANY)
    in_vmem = pl.BlockSpec(memory_space=pltpu.VMEM)
    summed, anchor_row, gradient, input_grad = pl.pallas_call(
        functools.partial(kernel, depth, groups, scale),
        out_shape=(
            jax.ShapeDtypeStruct((rows, cols), f32),
            jax.ShapeDtypeStruct((rows, width), bf16),
            jax.ShapeDtypeStruct((rows, width), f32),
            jax.ShapeDtypeStruct((tokens, width), bf16),
        ),
        in_specs=[any_space] * 5,
        out_specs=(in_vmem, in_vmem, in_vmem, any_space),
        scratch_shapes=[
            vmem((rows, cols), f32),
            vmem((rows, cols), f32),
            vmem((rows, width), f32),
            vmem((tokens, width), bf16),
            vmem((tokens, width), bf16),
            vmem((2 * rows, tokens), bf16),
            vmem((groups, rows, cols), bf16),
            vmem((groups - 1, rows, cols), bf16),
            vmem((depth, rows, rest), f32),
            vmem((depth, rows, rest), bf16),
            vmem((depth, rows, rest), bf16),
            vmem((depth, rows, rest), bf16),
            vmem((2 * depth, rows, rest), bf16),
            vmem((devices, rows, width), bf16),
            vmem((tokens, width), bf16),
            vmem((depth, 2 * rows, lead), f32),
            vmem((depth, 2 * rows, lead), bf16),
            vmem((2 * depth, 2 * rows, lead), bf16),
            vmem((rows, lead), bf16),
            vmem((rows, lead), bf16),
            dma((5,)), dma((depth,)),
            dma((groups - 1,)), dma((groups - 1,)),
            dma((2 * depth,)), dma((2 * depth,)),
            dma((depth,)), dma((2 * depth,)),
            dma((depth,)), dma((2 * depth,)), dma((1,)), dma((1,)),
            dma((depth - 1,)), dma((depth - 1,)),
            dma((depth,)), dma((depth,)),
            dma((2 * depth,)), dma((2 * depth,)),
            dma((4 * depth,)), dma((4 * depth,)),
        ],
        compiler_params=pltpu.CompilerParams(
            collective_id=0, has_side_effects=True, vmem_limit_bytes=60 * 2**20
        ),
    )(anchor, momentum, change[0], attn_out[0], grad_out[0])
    new_anchor, new_momentum = outer_step(anchor, momentum, summed, groups)
    local, first, second = adam(anchor_row.astype(f32), adam_first[0], adam_second[0], gradient)
    return new_anchor, new_momentum, local[None], first[None], second[None], input_grad[None]


def shards(*arrays):
    groups, devices = lax.axis_size("replica"), lax.axis_size("fsdp")
    rows, width = arrays[2].shape[1:]
    fits = (
        groups == 4 and devices % 2 == 0 and devices >= 4 and rows % 32 == 0
        and (2 * rows) % 128 == 0 and width % (128 * groups) == 0
        and lead_columns(width) > 0 and (width - lead_columns(width)) % 256 == 0
        and arrays[5].shape[1] * width <= 2**21
    )
    return (fused_shards if fits else plain_shards)(*arrays)


def solution(mesh):
    in_specs = (P("fsdp", "replica"),) * 2 + (P("replica", "fsdp", None),) * 5
    out_specs = (P("fsdp", "replica"),) * 2 + (P("replica", "fsdp", None),) * 4
    return jax.shard_map(shards, mesh=mesh, in_specs=in_specs, out_specs=out_specs, check_vma=False)
```
